32 devices in a mesh: tm: 8 (over y, x, core), freq: 4 (over z).
Axes of the slice: x: 2, y: 2, z: 4, core: 2. Of those that a mesh axis runs over, the one named last changes fastest.
Arguments:
- sfts: float32 [384, 2, 4096], P('tm', None, 'freq'), may hold values from -40 to 40
- detector_ids: int32 [384], replicated, may hold values from 0 to 2
- intersection: float32 [3, 3], replicated, may hold values from 0.3 to 1
- lags: int32 [12], replicated, may hold values from 1 to 16, as said below
- template_ids: int32 [4096, 2], P('tm'), may hold values from 0 to 63
Outputs:
- stat: float32 [4096, 4096], P('tm', 'freq')
The draws below stay inside these ranges and needn't reach their ends.
Inputs may be any that keep to these rules, and one draw needn't show every extreme that they name: 12 distinct lags, one of them 16.
All inputs are finite; a program needn't handle non-finite values.
Results may differ from the reference program's by a relative error of at most 0.009.
Values may be sent and summed in bfloat16 or wider, within the bound.
A program may use at most 64 MiB of HBM per device.

```python
import math
import jax
import jax.numpy as jnp
from jax import lax

NBIN = 4096
NTEMPL = 4096
LAGMAX = 16
NLAG = 12
NDET = 3
NGRID = 64
PERIOD = 283
SFT_DEV = 48
NSFT = 384


def draw_sfts(key, part):
    key_base = jax.random.fold_in(key, 11)
    key_rough = jax.random.fold_in(key, 12)
    key_rows = jax.random.fold_in(key, 13)
    bins = jnp.arange(NBIN, dtype=jnp.float32)
    ramp = jnp.exp(0.55 * bins / NBIN)
    rough = jax.random.uniform(key_rough, (NBIN,), jnp.float32, 0.6, 1.4)
    base = jnp.clip(jax.random.normal(key_base, (NSFT, 2, NBIN), jnp.float32), -6.0, 6.0)
    row_scale = jnp.exp(jax.random.uniform(key_rows, (NSFT,), jnp.float32, math.log(0.5), math.log(2.0)))
    values = base * row_scale[:, None, None] * (ramp * rough)[None, None, :]
    return jnp.clip(values, -40.0, 40.0).astype(jnp.float32)


def draw_lags(key, part):
    order = jax.random.permutation(jax.random.fold_in(key, 21), LAGMAX - 1)[:NLAG - 1].astype(jnp.int32) + 1
    return jnp.concatenate([jnp.full((1,), LAGMAX, jnp.int32), order])


def place_ends(array, stream_key, least, largest):
    longest = array.shape.index(max(array.shape))
    spots = []
    for shift in (0, 1):
        where = [jax.random.randint(jax.random.fold_in(stream_key, axis), (), 0, length) for axis, length in enumerate(array.shape)]
        where[longest] = (where[longest] + shift) % array.shape[longest]
        spots.append(tuple(where))
    return array.at[spots[0]].set(least).at[spots[1]].set(largest)


def setup_inputs(seed: int = 0) -> dict:
    key_list = jax.random.split(jax.random.key(seed), 6)
    sfts = draw_sfts(jax.random.fold_in(key_list[5], 71), 0)
    detector_ids = place_ends(jax.random.randint(key_list[1], (NSFT,), 0, NDET), jax.random.fold_in(key_list[1], 1), 0, NDET - 1).astype(jnp.int32)
    intersection = jnp.clip(jax.random.uniform(key_list[2], (NDET, NDET), jnp.float32, 0.3, 1.0), 0.3, 1.0)
    lags = draw_lags(jax.random.fold_in(key_list[5], 71), 0)
    template_ids = place_ends(jax.random.randint(key_list[4], (NTEMPL, 2), 0, NGRID), jax.random.fold_in(key_list[4], 1), 0, NGRID - 1).astype(jnp.int32)
    return {"sfts": sfts, "detector_ids": detector_ids, "intersection": intersection, "lags": lags, "template_ids": template_ids}


def block_term(extended, first_row, ids_padded, lag_list, intersection, amplitude_idx, phase_idx, total):
    span = extended.shape[0] - LAGMAX
    here = jnp.arange(span, dtype=jnp.int32)
    partner = here[None, :] + lag_list[:, None]
    own_rows = extended[:span].astype(jnp.float32)
    far_rows = extended[partner].astype(jnp.float32)
    det_block = lax.dynamic_slice_in_dim(ids_padded, first_row, extended.shape[0], 0)
    det_near = det_block[:span]
    det_far = det_block[partner]
    levels = jnp.arange(intersection.shape[0], dtype=jnp.int32)
    hot_near = (det_near[:, None] == levels[None, :]).astype(jnp.float32)
    hot_far = (det_far[:, :, None] == levels[None, None, :]).astype(jnp.float32)
    weight = jnp.einsum('sa,ab,lsb->ls', hot_near, intersection.astype(jnp.float32), hot_far)
    inside = first_row + partner < total
    weight = jnp.where(inside, weight, jnp.float32(0.0))
    re_own = own_rows[None, :, 0]
    im_own = own_rows[None, :, 1]
    re_far = far_rows[:, :, 0]
    im_far = far_rows[:, :, 1]
    pair_re = (weight[:, :, None] * (re_own * re_far + im_own * im_far)).astype(jnp.bfloat16)
    pair_im = (weight[:, :, None] * (re_own * im_far - im_own * re_far)).astype(jnp.bfloat16)
    width = extended.shape[2]
    stacked = jnp.concatenate([pair_re.reshape(-1, width), pair_im.reshape(-1, width)], 0)
    position = first_row + jnp.arange(extended.shape[0], dtype=jnp.int32)
    orbit = 2.0 * math.pi / PERIOD * (position % PERIOD).astype(jnp.float32)
    offset = 2.0 * math.pi / NGRID * phase_idx.astype(jnp.float32)
    sine = jnp.sin(offset[:, None] + orbit[None, :])
    amplitude = 8.0 + 4.0 * amplitude_idx.astype(jnp.float32)
    phase = amplitude[:, None, None] * (sine[:, partner] - sine[:, None, :span])
    rows = phase.shape[0]
    factors = jnp.concatenate([jnp.cos(phase).reshape(rows, -1).astype(jnp.bfloat16), jnp.sin(phase).reshape(rows, -1).astype(jnp.bfloat16)], 1)
    return jnp.dot(factors, stacked, preferred_element_type=jnp.float32)

def reference(sfts, detector_ids, intersection, lags, template_ids):
    power = lax.optimization_barrier(jnp.sum(sfts[:, 0] * sfts[:, 0] + sfts[:, 1] * sfts[:, 1], axis=1)) / NBIN
    white = (sfts * lax.rsqrt(power + 1e-06)[:, None, None]).astype(jnp.bfloat16)
    padded = jnp.pad(white, ((0, LAGMAX), (0, 0), (0, 0)))
    ids_padded = jnp.pad(detector_ids, (0, LAGMAX))
    total = sfts.shape[0]

    def add_block(number, totals):
        first_row = (number * SFT_DEV).astype(jnp.int32)
        extended = lax.dynamic_slice_in_dim(padded, first_row, SFT_DEV + LAGMAX, 0)
        return totals + block_term(extended, first_row, ids_padded, lags, intersection, template_ids[:, 0], template_ids[:, 1], total)
    totals = lax.fori_loop(0, total // SFT_DEV, add_block, jnp.zeros((NTEMPL, NBIN), jnp.float32))
    return totals * jnp.float32(1.0 / math.sqrt(total * NLAG))
```

```python
import functools
import math

import jax
import jax.numpy as jnp
import numpy as np
from jax import lax
from jax.experimental import pallas as pl
from jax.experimental.pallas import tpu as pltpu
from jax.sharding import PartitionSpec as P

NBIN = 4096
LAGMAX = 16
NGRID = 64
PERIOD = 283
PIECE = 256
MESH = pl.DeviceIdType.MESH


def even_series(function, degree):
    nodes = np.cos(np.pi * (np.arange(64) + 0.5) / 64) * 0.125 + 0.125
    fit = np.polynomial.chebyshev.Chebyshev.fit(nodes, function(np.sqrt(nodes)), degree, domain=[0, 0.25])
    return [float(c) for c in fit.convert(kind=np.polynomial.Polynomial).coef]


COS_SERIES = even_series(lambda y: np.cos(2 * np.pi * y), 7)


def horner(series, z):
    value = jnp.full_like(z, series[-1])
    for coefficient in series[-2::-1]:
        value = value * z + coefficient
    return value


def turn_cos(turns):
    y = turns - jnp.round(turns)
    return horner(COS_SERIES, y * y)


def xor(index, bits):
    out = index
    bit = 1
    while bit <= bits:
        if bits & bit:
            out = out + bit - 2 * bit * ((index // bit) % 2)
        bit *= 2
    return out


def bessel(argument, count):
    turn = np.arange(1024) * (2 * np.pi / 1024)
    wave = np.exp(1j * argument[..., None] * np.sin(turn))
    return np.real(np.fft.fft(wave, axis=-1) / 1024)[..., :count]


def argument_of(lag):
    return (8.0 + 4.0 * np.arange(NGRID)) * 2.0 * np.sin(np.pi * lag / PERIOD)


def harmonic_rows(nlag):
    rows = []
    for k in range(nlag):
        values = np.abs(bessel(argument_of(LAGMAX - nlag + 1 + k), 256))
        last = int(np.nonzero(values.max(axis=0) > 1e-5)[0].max())
        rows.append(-(-(last + 1) // 16) * 16)
    return rows


def row_harmonics(count):
    r = np.arange(count)
    even_n, even_s = 2 * ((r + 1) // 2), ((r > 0) & (r % 2 == 0)).astype(int)
    odd_n, odd_s = 2 * (r // 2) + 1, r % 2
    return np.concatenate([even_n, odd_n]), np.concatenate([even_s, odd_s])


def bessel_table(count, scale):
    n, _ = row_harmonics(count)
    values = np.stack([bessel(argument_of(lag), 256) for lag in range(1, LAGMAX + 1)])
    sign = np.where(n == 0, 1.0, 2.0) * np.where((n // 2) % 2 == 0, 1.0, -1.0) * scale
    table = (values[:, :, n] * sign).transpose(0, 2, 1)
    high = table.astype(jnp.bfloat16)
    low = (table - high.astype(np.float64)).astype(jnp.bfloat16)
    return np.concatenate([high, low], axis=2)


def kernel(
    n, nf, heads,
    x_ref, det_ref, inter_ref, lag_ref, tid_ref, bess_ref, out_ref,
    buf, pbuf, rbuf, rows_ref, shifted, weights, base, basis, bess, wave, factors, white, pairs, series, table_sem,
    bulk_send, bulk_recv, p_send, p_recv, r_send, r_recv,
):
    me = lax.axis_index("tm")
    mf = lax.axis_index("freq")
    span = x_ref.shape[0]
    rows = n * span
    nlag = lag_ref.shape[0]
    pieces = buf.shape[0]
    templ = tid_ref.shape[1]
    width = rows_ref.shape[2]
    most = base.shape[1]
    evens = [o for o in range(2, n, 2)]
    starts = [2 * sum(heads[:k]) for k in range(nlag + 1)]
    total_rows = starts[-1]

    table_copy = pltpu.make_async_copy(bess_ref, bess, table_sem)
    table_copy.start()

    re = x_ref[:, 0, :]
    im = x_ref[:, 1, :]
    for p in range(pieces):
        cols = slice(p * PIECE, (p + 1) * PIECE)
        buf[p, me, 0] = re[:, cols].astype(jnp.bfloat16)
        buf[p, me, 1] = im[:, cols].astype(jnp.bfloat16)
    local = jnp.sum(re * re + im * im, axis=1, keepdims=True)
    eye = lax.broadcasted_iota(jnp.int32, (span, 128), 0) == lax.broadcasted_iota(jnp.int32, (span, 128), 1)
    local_row = jnp.sum(jnp.where(eye, local, 0.0), axis=0, keepdims=True)
    pbuf[0] = jnp.broadcast_to(local_row, (8, 128))

    barrier = pltpu.get_barrier_semaphore()
    for d in range(1, nf):
        pl.semaphore_signal(barrier, inc=1, device_id=(me, (mf + d) % nf), device_id_type=MESH)
    for o in range(1, n):
        pl.semaphore_signal(barrier, inc=1, device_id=(xor(me, o), mf), device_id_type=MESH)
    pl.semaphore_wait(barrier, nf - 1 + n - 1)

    def power_copy(d):
        return pltpu.make_async_remote_copy(
            src_ref=pbuf.at[0], dst_ref=pbuf.at[d], send_sem=p_send.at[d], recv_sem=p_recv.at[d],
            device_id=(me, (mf + d) % nf), device_id_type=MESH)

    def rate_copy(o):
        return pltpu.make_async_remote_copy(
            src_ref=rbuf.at[me], dst_ref=rbuf.at[me], send_sem=r_send.at[o], recv_sem=r_recv.at[o],
            device_id=(xor(me, o), mf), device_id_type=MESH)

    def own_copy(p, o):
        return pltpu.make_async_remote_copy(
            src_ref=buf.at[p, me], dst_ref=buf.at[p, me], send_sem=bulk_send.at[p, o], recv_sem=bulk_recv.at[p, o],
            device_id=(xor(me, o), mf), device_id_type=MESH)

    def pass_copy(p, o):
        block = xor(me, o)
        return pltpu.make_async_remote_copy(
            src_ref=buf.at[p, block], dst_ref=buf.at[p, block],
            send_sem=bulk_send.at[p, o + 1], recv_sem=bulk_recv.at[p, o + 1],
            device_id=(xor(me, 1), mf), device_id_type=MESH)

    def landed(p, o):
        block = xor(me, o)
        pltpu.make_async_remote_copy(
            src_ref=buf.at[p, block], dst_ref=buf.at[p, block],
            send_sem=bulk_send.at[p, o], recv_sem=bulk_recv.at[p, o],
            device_id=(xor(me, o), mf), device_id_type=MESH).wait_recv()

    for d in range(1, nf):
        power_copy(d).start()
    for p in range(pieces):
        for o in evens + [1]:
            own_copy(p, o).start()

    lag = [lag_ref[l] for l in range(nlag)]
    for turn in range(nlag):
        for l in range(turn % 2, nlag - 1, 2):
            lag[l], lag[l + 1] = jnp.minimum(lag[l], lag[l + 1]), jnp.maximum(lag[l], lag[l + 1])
    lag = [jnp.maximum(value, 1) for value in lag]

    def harmonics(count, lanes):
        r = lax.broadcasted_iota(jnp.int32, (count, lanes), 0)
        even_n = 2 * ((r + 1) // 2)
        even_s = jnp.where(r > 0, 1 - r % 2, 0)
        odd_n = 2 * (r // 2) + 1
        odd_s = r % 2
        return [(a.astype(jnp.float32), b.astype(jnp.float32)) for a, b in ((even_n, even_s), (odd_n, odd_s))]

    for c in range(rows // 128):
        index = (lax.broadcasted_iota(jnp.int32, (most, 128), 1) + c * 128).astype(jnp.float32)
        position = index - PERIOD * jnp.floor((index + 0.5) * (1.0 / PERIOD))
        for parity, (harmonic, quarter) in enumerate(harmonics(most, 128)):
            steps = harmonic * position
            steps = steps - PERIOD * jnp.floor((steps + 0.5) * (1.0 / PERIOD))
            base[parity, :, c * 128:(c + 1) * 128] = turn_cos(steps * (1.0 / PERIOD) - 0.25 * quarter)

    lane = lax.broadcasted_iota(jnp.int32, (1, 2 * NGRID), 1)
    level = (lane % NGRID).astype(jnp.float32)
    for k in range(nlag):
        for parity, (harmonic, quarter) in enumerate(harmonics(heads[k], 2 * NGRID)):
            turns = harmonic * (level * (1.0 / NGRID))
            turns = turns - jnp.round(turns)
            half = harmonic * lag[k].astype(jnp.float32) * (0.5 / PERIOD)
            half = half - jnp.round(half)
            value = turn_cos(turns + half + 0.25 * quarter)
            high = value.astype(jnp.bfloat16).astype(jnp.float32)
            start = starts[k] + parity * heads[k]
            wave[start:start + heads[k], :] = jnp.where(lane < NGRID, high, value - high).astype(jnp.bfloat16)

    rows_ref[0] = jnp.full((8, width), -1.0, jnp.float32)
    for c in range(rows // 128):
        ids = det_ref[c * 128:(c + 1) * 128].astype(jnp.float32)[None, :]
        rows_ref[0, :, c * 128:(c + 1) * 128] = jnp.broadcast_to(ids, (8, 128))
    det_row = rows_ref[0, 0:1, :]
    for v in range(1, LAGMAX + 1):
        shifted[v - 1:v, :] = pltpu.roll(det_row, width - v, 1)
    near = det_row[:, :rows]
    far = shifted[:, :rows]
    ndet = inter_ref.shape[0]
    gains = jnp.zeros((LAGMAX, rows), jnp.float32)
    for b in range(ndet):
        gain = jnp.zeros((1, rows), jnp.float32)
        for a in range(ndet):
            gain = jnp.where(near == a, inter_ref[a, b], gain)
        gains = jnp.where(far == b, gain, gains)
    weights[...] = gains

    for h in range(PIECE // 128):
        white[:, h, rows:rows + LAGMAX, :] = jnp.zeros((2, LAGMAX, 128), jnp.float32)

    def forward(p):
        for o in evens:
            landed(p, o)
            pass_copy(p, o).start()

    for d in range(1, nf):
        power_copy(d).wait_recv()
    total = pbuf[0]
    for d in range(1, nf):
        total = total + pbuf[d]
    rbuf[me] = lax.rsqrt(total * (1.0 / NBIN) + 1e-06)
    for o in range(1, n):
        rate_copy(o).start()

    table_copy.wait()
    for k in range(nlag):
        for parity in range(2):
            start = starts[k] + parity * heads[k]
            series[start:start + heads[k], 0:2 * NGRID] = bess[lag[k] - 1, parity * most:parity * most + heads[k], :]
    grid_row = lax.broadcasted_iota(jnp.int32, (2 * NGRID, templ), 0) % NGRID
    pick_amplitude = (grid_row == tid_ref[0:1, :]).astype(jnp.float32).T.astype(jnp.bfloat16)
    pick_phase = (grid_row == tid_ref[1:2, :]).astype(jnp.float32).T.astype(jnp.bfloat16)
    contract = (((1,), (1,)), ((), ()))
    step = 256
    for c in range(total_rows // step):
        here = slice(c * step, (c + 1) * step)
        bessel_part = lax.dot_general(
            pick_amplitude, series[here, 0:2 * NGRID], contract, preferred_element_type=jnp.float32)
        wave_part = lax.dot_general(pick_phase, wave[here, :], contract, preferred_element_type=jnp.float32)
        factors[:, here] = (bessel_part * wave_part).astype(jnp.bfloat16)

    forward(0)

    for o in range(1, n):
        pltpu.make_async_remote_copy(
            src_ref=rbuf.at[xor(me, o)], dst_ref=rbuf.at[xor(me, o)], send_sem=r_send.at[o], recv_sem=r_recv.at[o],
            device_id=(xor(me, o), mf), device_id_type=MESH).wait_recv()
    valid = lax.broadcasted_iota(jnp.int32, (1, width), 1) < span
    rate_row = jnp.zeros((1, width), jnp.float32)
    for g in range(n):
        part = jnp.concatenate([rbuf[g, 0:1, :], jnp.zeros((1, width - 128), jnp.float32)], axis=1)
        part = jnp.where(valid, part, 0.0)
        rate_row = rate_row + (pltpu.roll(part, g * span, 1) if g else part)
    for v in range(1, LAGMAX + 1):
        shifted[v - 1:v, :] = pltpu.roll(rate_row, width - v, 1)
    weights[...] = weights[...] * (rate_row[:, :rows] * shifted[:, :rows])
    for k in range(nlag):
        weight = weights[pl.ds(lag[k] - 1, 1), :]
        for parity in range(2):
            start = starts[k] + parity * heads[k]
            basis[start:start + heads[k], :] = (base[parity, :heads[k], :] * weight).astype(jnp.bfloat16)

    chunk = 48

    def piece_step(p, carry):
        for o in range(1, n, 2):
            landed(p, o)

        @pl.when(p + 1 < pieces)
        def _():
            forward(p + 1)

        for g in range(n):
            here = slice(g * span, (g + 1) * span)
            for c in range(2):
                for h in range(PIECE // 128):
                    white[c, h, here, :] = buf[p, g, c, :, h * 128:(h + 1) * 128].astype(jnp.float32)

        for k in range(nlag):
            for r in range(rows // chunk):
                here = slice(r * chunk, (r + 1) * chunk)
                there = pl.ds(r * chunk + lag[k], chunk)
                for h in range(PIECE // 128):
                    cols = slice(h * 128, (h + 1) * 128)
                    a = white[0, h, here, :]
                    b = white[1, h, here, :]
                    c = white[0, h, there, :]
                    d = white[1, h, there, :]
                    pairs[k % 2, 0, here, cols] = (a * c + b * d).astype(jnp.bfloat16)
                    pairs[k % 2, 1, here, cols] = (a * d - b * c).astype(jnp.bfloat16)
            for parity in range(2):
                start = starts[k] + parity * heads[k]
                series[start:start + heads[k], :] = jnp.dot(
                    basis[start:start + heads[k], :], pairs[k % 2, parity],
                    preferred_element_type=jnp.float32).astype(jnp.bfloat16)
        product = jnp.dot(factors[...], series[...], preferred_element_type=jnp.float32)
        out_ref[:, pl.ds(pl.multiple_of(p * PIECE, PIECE), PIECE)] = product.astype(out_ref.dtype)
        return carry

    lax.fori_loop(0, pieces, piece_step, 0)

    for d in range(1, nf):
        power_copy(d).wait_send()
    for o in range(1, n):
        rate_copy(o).wait_send()

    def drain(p, carry):
        for o in evens + [1]:
            own_copy(p, o).wait_send()
        for o in evens:
            pass_copy(p, o).wait_send()
        return carry

    lax.fori_loop(0, pieces, drain, 0)


def shards(n, nf, sfts, detector_ids, intersection, lags, template_ids):
    span, _, width = sfts.shape
    rows = detector_ids.shape[0]
    nlag = lags.shape[0]
    templ = template_ids.shape[0]
    pieces = width // PIECE
    heads = harmonic_rows(nlag)
    most = max(heads)
    total_rows = 2 * sum(heads)
    table = jnp.asarray(bessel_table(most, 1.0 / math.sqrt(rows * nlag)))
    lanes = rows + 128
    vmem = pl.BlockSpec(memory_space=pltpu.VMEM)
    smem = pl.BlockSpec(memory_space=pltpu.SMEM)
    stat = pl.pallas_call(
        functools.partial(kernel, n, nf, heads),
        out_shape=jax.ShapeDtypeStruct((templ, width), jnp.bfloat16),
        in_specs=[vmem, vmem, smem, smem, vmem, pl.BlockSpec(memory_space=pl.ANY)],
        out_specs=vmem,
        scratch_shapes=[
            pltpu.VMEM((pieces, n, 2, span, PIECE), jnp.bfloat16),
            pltpu.VMEM((nf, 8, 128), jnp.float32),
            pltpu.VMEM((n, 8, 128), jnp.float32),
            pltpu.VMEM((1, 8, lanes), jnp.float32),
            pltpu.VMEM((LAGMAX, lanes), jnp.float32),
            pltpu.VMEM((LAGMAX, rows), jnp.float32),
            pltpu.VMEM((2, most, rows), jnp.float32),
            pltpu.VMEM((total_rows, rows), jnp.bfloat16),
            pltpu.VMEM(table.shape, jnp.bfloat16),
            pltpu.VMEM((total_rows, 2 * NGRID), jnp.bfloat16),
            pltpu.VMEM((templ, total_rows), jnp.bfloat16),
            pltpu.VMEM((2, PIECE // 128, rows + LAGMAX, 128), jnp.float32),
            pltpu.VMEM((2, 2, rows, PIECE), jnp.bfloat16),
            pltpu.VMEM((total_rows, PIECE), jnp.bfloat16),
            pltpu.SemaphoreType.DMA(()),
            pltpu.SemaphoreType.DMA((pieces, n)),
            pltpu.SemaphoreType.DMA((pieces, n)),
            pltpu.SemaphoreType.DMA((nf,)),
            pltpu.SemaphoreType.DMA((nf,)),
            pltpu.SemaphoreType.DMA((n,)),
            pltpu.SemaphoreType.DMA((n,)),
        ],
        compiler_params=pltpu.CompilerParams(
            collective_id=0, has_side_effects=True, vmem_limit_bytes=60 * 1024 * 1024
        ),
    )(sfts, detector_ids, intersection, lags, template_ids.T, table)
    return stat.astype(jnp.float32)


def solution(mesh):
    n, nf = mesh.shape["tm"], mesh.shape["freq"]
    in_specs = (P("tm", None, "freq"), P(), P(), P(), P("tm", None))
    return jax.shard_map(
        functools.partial(shards, n, nf), mesh=mesh, in_specs=in_specs, out_specs=P("tm", "freq"), check_vma=False
    )
```

```python
import functools
import math

import jax
import jax.numpy as jnp
import numpy as np
from jax import lax
from jax.experimental import pallas as pl
from jax.experimental.pallas import tpu as pltpu
from jax.sharding import PartitionSpec as P

NBIN = 4096
LAGMAX = 16
NGRID = 64
PERIOD = 283
PIECE = 256
MESH = pl.DeviceIdType.MESH


def even_series(function, degree):
    nodes = np.cos(np.pi * (np.arange(64) + 0.5) / 64) * 0.125 + 0.125
    fit = np.polynomial.chebyshev.Chebyshev.fit(nodes, function(np.sqrt(nodes)), degree, domain=[0, 0.25])
    return [float(c) for c in fit.convert(kind=np.polynomial.Polynomial).coef]


COS_SERIES = even_series(lambda y: np.cos(2 * np.pi * y), 7)


def horner(series, z):
    value = jnp.full_like(z, series[-1])
    for coefficient in series[-2::-1]:
        value = value * z + coefficient
    return value


def turn_cos(turns):
    y = turns - jnp.round(turns)
    return horner(COS_SERIES, y * y)


def xor(index, bits):
    out = index
    bit = 1
    while bit <= bits:
        if bits & bit:
            out = out + bit - 2 * bit * ((index // bit) % 2)
        bit *= 2
    return out


def bessel(argument, count):
    turn = np.arange(1024) * (2 * np.pi / 1024)
    wave = np.exp(1j * argument[..., None] * np.sin(turn))
    return np.real(np.fft.fft(wave, axis=-1) / 1024)[..., :count]


def argument_of(lag):
    return (8.0 + 4.0 * np.arange(NGRID)) * 2.0 * np.sin(np.pi * lag / PERIOD)


def harmonic_rows(nlag):
    rows = []
    for k in range(nlag):
        values = np.abs(bessel(argument_of(LAGMAX - nlag + 1 + k), 256))
        last = int(np.nonzero(values.max(axis=0) > 1e-5)[0].max())
        rows.append(-(-(last + 1) // 16) * 16)
    return rows


def row_harmonics(count):
    r = np.arange(count)
    even_n, even_s = 2 * ((r + 1) // 2), ((r > 0) & (r % 2 == 0)).astype(int)
    odd_n, odd_s = 2 * (r // 2) + 1, r % 2
    return np.concatenate([even_n, odd_n]), np.concatenate([even_s, odd_s])


def bessel_table(count, scale):
    n, _ = row_harmonics(count)
    values = np.stack([bessel(argument_of(lag), 256) for lag in range(1, LAGMAX + 1)])
    sign = np.where(n == 0, 1.0, 2.0) * np.where((n // 2) % 2 == 0, 1.0, -1.0) * scale
    table = (values[:, :, n] * sign).transpose(0, 2, 1)
    high = table.astype(jnp.bfloat16)
    low = (table - high.astype(np.float64)).astype(jnp.bfloat16)
    return np.concatenate([high, low], axis=2)


def kernel(
    n, nf, heads,
    x_hbm, det_hbm, inter_hbm, lag_hbm, tid_hbm, bess_hbm, out_ref,
    x_ref, det_ref, inter_ref, lag_ref, tid_ref,
    buf, pbuf, rows_ref, shifted, weights, base, basis, bess, wave, picked, factors, white, near_rows, series, load_sem,
    bulk_send, bulk_recv, p_send, p_recv, r_send, r_recv,
):
    me = lax.axis_index("tm")
    mf = lax.axis_index("freq")
    span = x_ref.shape[0]
    rows = n * span
    nlag = lag_ref.shape[0]
    pieces = buf.shape[0]
    templ = tid_ref.shape[1]
    width = rows_ref.shape[2]
    most = base.shape[1]
    evens = sorted(range(2, n, 2), key=lambda o: -bin(o).count("1"))
    starts = [2 * sum(heads[:k]) for k in range(nlag + 1)]
    total_rows = starts[-1]

    loads = [
        pltpu.make_async_copy(source, target, load_sem.at[i])
        for i, (source, target) in enumerate([
            (x_hbm, x_ref), (lag_hbm, lag_ref), (det_hbm, det_ref), (tid_hbm, tid_ref), (inter_hbm, inter_ref),
            (bess_hbm, bess)])
    ]
    for load in loads:
        load.start()
    barrier = pltpu.get_barrier_semaphore()
    for d in range(1, nf):
        pl.semaphore_signal(barrier, inc=1, device_id=(me, (mf + d) % nf), device_id_type=MESH)
    for o in range(1, n):
        pl.semaphore_signal(barrier, inc=1, device_id=(xor(me, o), mf), device_id_type=MESH)

    loads[0].wait()
    re = x_ref[:, 0, :]
    im = x_ref[:, 1, :]
    local = jnp.sum(re * re + im * im, axis=1, keepdims=True)
    eye = lax.broadcasted_iota(jnp.int32, (span, 128), 0) == lax.broadcasted_iota(jnp.int32, (span, 128), 1)
    pbuf[0, pl.ds(me, 1), :] = jnp.sum(jnp.where(eye, local, 0.0), axis=0, keepdims=True)
    for p in range(pieces):
        for h in range(PIECE // 128):
            cols = slice(p * PIECE + h * 128, p * PIECE + (h + 1) * 128)
            buf[p, me, 0, h] = re[:, cols].astype(jnp.bfloat16)
            buf[p, me, 1, h] = im[:, cols].astype(jnp.bfloat16)
    pl.semaphore_wait(barrier, nf - 1 + n - 1)

    def share_copy(o, block):
        return pltpu.make_async_remote_copy(
            src_ref=pbuf.at[0, pl.ds(block, 1)], dst_ref=pbuf.at[0, pl.ds(block, 1)],
            send_sem=r_send.at[o], recv_sem=r_recv.at[o],
            device_id=(xor(me, o), mf), device_id_type=MESH)

    def power_copy(d):
        return pltpu.make_async_remote_copy(
            src_ref=pbuf.at[0], dst_ref=pbuf.at[d], send_sem=p_send.at[d], recv_sem=p_recv.at[d],
            device_id=(me, (mf + d) % nf), device_id_type=MESH)

    def own_copy(p, o):
        return pltpu.make_async_remote_copy(
            src_ref=buf.at[p, me], dst_ref=buf.at[p, me], send_sem=bulk_send.at[p, o], recv_sem=bulk_recv.at[p, o],
            device_id=(xor(me, o), mf), device_id_type=MESH)

    def pass_copy(p, o):
        block = xor(me, o)
        return pltpu.make_async_remote_copy(
            src_ref=buf.at[p, block], dst_ref=buf.at[p, block],
            send_sem=bulk_send.at[p, o + 1], recv_sem=bulk_recv.at[p, o + 1],
            device_id=(xor(me, 1), mf), device_id_type=MESH)

    def landed(p, o):
        block = xor(me, o)
        pltpu.make_async_remote_copy(
            src_ref=buf.at[p, block], dst_ref=buf.at[p, block],
            send_sem=bulk_send.at[p, o], recv_sem=bulk_recv.at[p, o],
            device_id=(xor(me, o), mf), device_id_type=MESH).wait_recv()

    for o in evens + [1] + list(range(3, n, 2)):
        share_copy(o, me).start()
    for p in range(pieces):
        for o in evens + [1]:
            own_copy(p, o).start()

    for load in loads[1:5]:
        load.wait()
    lag = [lag_ref[l] for l in range(nlag)]
    for turn in range(nlag):
        for l in range(turn % 2, nlag - 1, 2):
            lag[l], lag[l + 1] = jnp.minimum(lag[l], lag[l + 1]), jnp.maximum(lag[l], lag[l + 1])
    lag = [jnp.maximum(value, 1) for value in lag]

    def harmonics(count, lanes):
        r = lax.broadcasted_iota(jnp.int32, (count, lanes), 0)
        even_n = 2 * ((r + 1) // 2)
        even_s = jnp.where(r > 0, 1 - r % 2, 0)
        odd_n = 2 * (r // 2) + 1
        odd_s = r % 2
        return [(a.astype(jnp.float32), b.astype(jnp.float32)) for a, b in ((even_n, even_s), (odd_n, odd_s))]

    for c in range(rows // 128):
        index = (lax.broadcasted_iota(jnp.int32, (most, 128), 1) + c * 128).astype(jnp.float32)
        position = index - PERIOD * jnp.floor((index + 0.5) * (1.0 / PERIOD))
        for parity, (harmonic, quarter) in enumerate(harmonics(most, 128)):
            steps = harmonic * position
            steps = steps - PERIOD * jnp.floor((steps + 0.5) * (1.0 / PERIOD))
            base[parity, :, c * 128:(c + 1) * 128] = turn_cos(steps * (1.0 / PERIOD) - 0.25 * quarter)

    lane = lax.broadcasted_iota(jnp.int32, (1, 2 * NGRID), 1)
    level = (lane % NGRID).astype(jnp.float32)
    for k in range(nlag):
        for parity, (harmonic, quarter) in enumerate(harmonics(heads[k], 2 * NGRID)):
            turns = harmonic * (level * (1.0 / NGRID))
            turns = turns - jnp.round(turns)
            half = harmonic * lag[k].astype(jnp.float32) * (0.5 / PERIOD)
            half = half - jnp.round(half)
            value = turn_cos(turns + half + 0.25 * quarter)
            high = value.astype(jnp.bfloat16).astype(jnp.float32)
            start = starts[k] + parity * heads[k]
            wave[start:start + heads[k], :] = jnp.where(lane < NGRID, high, value - high).astype(jnp.bfloat16)

    rows_ref[0] = jnp.full((8, width), -1.0, jnp.float32)
    for c in range(rows // 128):
        ids = det_ref[c * 128:(c + 1) * 128].astype(jnp.float32)[None, :]
        rows_ref[0, :, c * 128:(c + 1) * 128] = jnp.broadcast_to(ids, (8, 128))
    det_row = rows_ref[0, 0:1, :]
    for v in range(1, LAGMAX + 1):
        shifted[v - 1:v, :] = pltpu.roll(det_row, width - v, 1)
    near = det_row[:, :rows]
    far = shifted[:, :rows]
    ndet = inter_ref.shape[0]
    gains = jnp.zeros((LAGMAX, rows), jnp.float32)
    for b in range(ndet):
        gain = jnp.zeros((1, rows), jnp.float32)
        for a in range(ndet):
            gain = jnp.where(near == a, inter_ref[a, b], gain)
        gains = jnp.where(far == b, gain, gains)
    weights[...] = gains

    for h in range(PIECE // 128):
        white[:, h, rows:rows + LAGMAX, :] = jnp.zeros((2, LAGMAX, 128), jnp.float32)

    def forward(p):
        for o in evens[::-1]:
            landed(p, o)
            pass_copy(p, o).start()

    for o in range(1, n):
        share_copy(o, xor(me, o)).wait_recv()
    for d in range(1, nf):
        power_copy(d).start()

    loads[5].wait()
    for k in range(nlag):
        for parity in range(2):
            start = starts[k] + parity * heads[k]
            picked[start:start + heads[k], :] = bess[lag[k] - 1, parity * most:parity * most + heads[k], :]
    grid_row = lax.broadcasted_iota(jnp.int32, (2 * NGRID, templ), 0) % NGRID
    pick_amplitude = (grid_row == tid_ref[0:1, :]).astype(jnp.float32).T.astype(jnp.bfloat16)
    pick_phase = (grid_row == tid_ref[1:2, :]).astype(jnp.float32).T.astype(jnp.bfloat16)
    contract = (((1,), (1,)), ((), ()))
    step = 256
    for c in range(total_rows // step):
        here = slice(c * step, (c + 1) * step)
        bessel_part = lax.dot_general(
            pick_amplitude, picked[here, :], contract, preferred_element_type=jnp.float32)
        wave_part = lax.dot_general(pick_phase, wave[here, :], contract, preferred_element_type=jnp.float32)
        product = bessel_part * wave_part
        for h in range(step // 128):
            factors[c * (step // 128) + h] = product[:, h * 128:(h + 1) * 128].astype(jnp.bfloat16)

    forward(0)

    total = pbuf[0]
    for d in range(1, nf):
        power_copy(d).wait_recv()
        total = total + pbuf[d]
    rates = lax.rsqrt(total * (1.0 / NBIN) + 1e-06)
    rates = jnp.where(lax.broadcasted_iota(jnp.int32, (n, 128), 1) < span, rates, 0.0)
    rates = jnp.concatenate([rates, jnp.zeros((n, width - 128), jnp.float32)], axis=1)
    rate_row = rates[0:1]
    for g in range(1, n):
        rate_row = rate_row + pltpu.roll(rates[g:g + 1], g * span, 1)
    for v in range(1, LAGMAX + 1):
        shifted[v - 1:v, :] = pltpu.roll(rate_row, width - v, 1)
    weights[...] = weights[...] * (rate_row[:, :rows] * shifted[:, :rows])
    for k in range(nlag):
        weight = weights[pl.ds(lag[k] - 1, 1), :]
        for parity in range(2):
            start = starts[k] + parity * heads[k]
            for c in range(rows // 128):
                cols = slice(c * 128, (c + 1) * 128)
                basis[c, start:start + heads[k], :] = (base[parity, :heads[k], cols] * weight[:, cols]).astype(jnp.bfloat16)

    def piece_step(p, carry):
        for o in range(1, n, 2):
            landed(p, o)

        for g in range(n):
            here = slice(g * span, (g + 1) * span)
            for c in range(2):
                for h in range(PIECE // 128):
                    white[c, h, here, :] = buf[p, g, c, h].astype(jnp.float32)
                    near_rows[c, h, here, :] = buf[p, g, c, h]

        for k in range(nlag):
            if k == nlag // 2:
                @pl.when(p + 1 < pieces)
                def _():
                    forward(p + 1)

            there = pl.ds(lag[k], rows)
            a, b = [jnp.concatenate([near_rows[part, h] for h in range(PIECE // 128)], axis=1) for part in range(2)]
            c, d = [
                jnp.concatenate([white[part, h, there, :] for h in range(PIECE // 128)], axis=1).astype(jnp.bfloat16)
                for part in range(2)]
            for parity in range(2):
                start = starts[k] + parity * heads[k]
                both = a * d - b * c if parity else a * c + b * d
                piece = jnp.dot(
                    jnp.concatenate([basis[c, start:start + heads[k], :] for c in range(rows // 128)], axis=1),
                    both, preferred_element_type=jnp.float32)
                for h in range(PIECE // 128):
                    series[h, start:start + heads[k], :] = piece[:, h * 128:(h + 1) * 128].astype(jnp.bfloat16)
        product = jnp.dot(
            jnp.concatenate([factors[c] for c in range(total_rows // 128)], axis=1),
            jnp.concatenate([series[h] for h in range(PIECE // 128)], axis=1), preferred_element_type=jnp.float32)
        out_ref[:, pl.ds(pl.multiple_of(p * PIECE, PIECE), PIECE)] = product.astype(out_ref.dtype)
        return carry

    lax.fori_loop(0, pieces, piece_step, 0)

    for d in range(1, nf):
        power_copy(d).wait_send()
    for o in range(1, n):
        share_copy(o, me).wait_send()

    def drain(p, carry):
        for o in evens + [1]:
            own_copy(p, o).wait_send()
        for o in evens:
            pass_copy(p, o).wait_send()
        return carry

    lax.fori_loop(0, pieces, drain, 0)


def shards(n, nf, sfts, detector_ids, intersection, lags, template_ids):
    span, _, width = sfts.shape
    rows = detector_ids.shape[0]
    nlag = lags.shape[0]
    templ = template_ids.shape[0]
    pieces = width // PIECE
    heads = harmonic_rows(nlag)
    most = max(heads)
    total_rows = 2 * sum(heads)
    table = jnp.asarray(bessel_table(most, 1.0 / math.sqrt(rows * nlag)))
    lanes = rows + 128
    vmem = pl.BlockSpec(memory_space=pltpu.VMEM)
    operands = [
        pltpu.with_memory_space_constraint(operand, pltpu.HBM)
        for operand in (sfts, detector_ids, intersection, lags, template_ids.T, table)
    ]
    return pl.pallas_call(
        functools.partial(kernel, n, nf, heads),
        out_shape=pltpu.VMEM((templ, width), jnp.float32),
        in_specs=[pl.BlockSpec(memory_space=pltpu.HBM)] * 6,
        out_specs=vmem,
        scratch_shapes=[
            pltpu.VMEM(sfts.shape, jnp.float32),
            pltpu.VMEM((rows,), jnp.int32),
            pltpu.SMEM(intersection.shape, jnp.float32),
            pltpu.SMEM((nlag,), jnp.int32),
            pltpu.VMEM((2, templ), jnp.int32),
            pltpu.VMEM((pieces, n, 2, PIECE // 128, span, 128), jnp.bfloat16),
            pltpu.VMEM((nf, n, 128), jnp.float32),
            pltpu.VMEM((1, 8, lanes), jnp.float32),
            pltpu.VMEM((LAGMAX, lanes), jnp.float32),
            pltpu.VMEM((LAGMAX, rows), jnp.float32),
            pltpu.VMEM((2, most, rows), jnp.float32),
            pltpu.VMEM((rows // 128, total_rows, 128), jnp.bfloat16),
            pltpu.VMEM(table.shape, jnp.bfloat16),
            pltpu.VMEM((total_rows, 2 * NGRID), jnp.bfloat16),
            pltpu.VMEM((total_rows, 2 * NGRID), jnp.bfloat16),
            pltpu.VMEM((total_rows // 128, templ, 128), jnp.bfloat16),
            pltpu.VMEM((2, PIECE // 128, rows + LAGMAX, 128), jnp.float32),
            pltpu.VMEM((2, PIECE // 128, rows, 128), jnp.bfloat16),
            pltpu.VMEM((PIECE // 128, total_rows, 128), jnp.bfloat16),
            pltpu.SemaphoreType.DMA((6,)),
            pltpu.SemaphoreType.DMA((pieces, n)),
            pltpu.SemaphoreType.DMA((pieces, n)),
            pltpu.SemaphoreType.DMA((nf,)),
            pltpu.SemaphoreType.DMA((nf,)),
            pltpu.SemaphoreType.DMA((n,)),
            pltpu.SemaphoreType.DMA((n,)),
        ],
        compiler_params=pltpu.CompilerParams(
            collective_id=0, has_side_effects=True, vmem_limit_bytes=48 * 1024 * 1024
        ),
    )(*operands)


def solution(mesh):
    n, nf = mesh.shape["tm"], mesh.shape["freq"]
    in_specs = (P("tm", None, "freq"), P(), P(), P(), P("tm", None))
    return jax.shard_map(
        functools.partial(shards, n, nf), mesh=mesh, in_specs=in_specs, out_specs=P("tm", "freq"), check_vma=False
    )
```

```python
import functools
import math

import jax
import jax.numpy as jnp
import numpy as np
from jax import lax
from jax.experimental import pallas as pl
from jax.experimental.pallas import tpu as pltpu
from jax.sharding import PartitionSpec as P

NBIN = 4096
LAGMAX = 16
NGRID = 64
PERIOD = 283
PIECE = 256
MESH = pl.DeviceIdType.MESH


def even_series(function, degree):
    nodes = np.cos(np.pi * (np.arange(64) + 0.5) / 64) * 0.125 + 0.125
    fit = np.polynomial.chebyshev.Chebyshev.fit(nodes, function(np.sqrt(nodes)), degree, domain=[0, 0.25])
    return [float(c) for c in fit.convert(kind=np.polynomial.Polynomial).coef]


COS_SERIES = even_series(lambda y: np.cos(2 * np.pi * y), 7)


def horner(series, z):
    value = jnp.full_like(z, series[-1])
    for coefficient in series[-2::-1]:
        value = value * z + coefficient
    return value


def turn_cos(turns):
    y = turns - jnp.round(turns)
    return horner(COS_SERIES, y * y)


def xor(index, bits):
    out = index
    bit = 1
    while bit <= bits:
        if bits & bit:
            out = out + bit - 2 * bit * ((index // bit) % 2)
        bit *= 2
    return out


def bessel(argument, count):
    turn = np.arange(1024) * (2 * np.pi / 1024)
    wave = np.exp(1j * argument[..., None] * np.sin(turn))
    return np.real(np.fft.fft(wave, axis=-1) / 1024)[..., :count]


def argument_of(lag):
    return (8.0 + 4.0 * np.arange(NGRID)) * 2.0 * np.sin(np.pi * lag / PERIOD)


def harmonic_rows(nlag):
    rows = []
    for k in range(nlag):
        values = np.abs(bessel(argument_of(LAGMAX - nlag + 1 + k), 256))
        last = int(np.nonzero(values.max(axis=0) > 1e-5)[0].max())
        rows.append(-(-(last + 1) // 16) * 16)
    return rows


def row_harmonics(count):
    r = np.arange(count)
    even_n, even_s = 2 * ((r + 1) // 2), ((r > 0) & (r % 2 == 0)).astype(int)
    odd_n, odd_s = 2 * (r // 2) + 1, r % 2
    return np.concatenate([even_n, odd_n]), np.concatenate([even_s, odd_s])


def bessel_table(count, scale):
    n, _ = row_harmonics(count)
    values = np.stack([bessel(argument_of(lag), 256) for lag in range(1, LAGMAX + 1)])
    sign = np.where(n == 0, 1.0, 2.0) * np.where((n // 2) % 2 == 0, 1.0, -1.0) * scale
    table = (values[:, :, n] * sign).transpose(0, 2, 1)
    high = table.astype(jnp.bfloat16)
    low = (table - high.astype(np.float64)).astype(jnp.bfloat16)
    return np.concatenate([high, low], axis=2)


def kernel(
    n, nf, heads,
    x_hbm, det_hbm, inter_hbm, lag_hbm, tid_hbm, bess_hbm, out_ref,
    x_ref, det_ref, inter_ref, lag_ref, tid_ref,
    buf, pbuf, rows_ref, shifted, weights, base, basis, bess, wave, picked, factors, white, near_rows, series, load_sem,
    bulk_send, bulk_recv, p_send, p_recv, r_send, r_recv,
):
    me = lax.axis_index("tm")
    mf = lax.axis_index("freq")
    span = x_ref.shape[0]
    rows = n * span
    nlag = lag_ref.shape[0]
    pieces = buf.shape[0]
    templ = tid_ref.shape[1]
    width = rows_ref.shape[2]
    most = base.shape[1]
    evens = sorted(range(2, n, 2), key=lambda o: -bin(o).count("1"))
    starts = [2 * sum(heads[:k]) for k in range(nlag + 1)]
    total_rows = starts[-1]

    loads = [
        pltpu.make_async_copy(source, target, load_sem.at[i])
        for i, (source, target) in enumerate([
            (x_hbm, x_ref), (lag_hbm, lag_ref), (det_hbm, det_ref), (tid_hbm, tid_ref), (inter_hbm, inter_ref),
            (bess_hbm, bess)])
    ]
    for load in loads:
        load.start()
    barrier = pltpu.get_barrier_semaphore()
    for d in range(1, nf):
        pl.semaphore_signal(barrier, inc=1, device_id=(me, (mf + d) % nf), device_id_type=MESH)
    for o in range(1, n):
        pl.semaphore_signal(barrier, inc=1, device_id=(xor(me, o), mf), device_id_type=MESH)

    loads[0].wait()
    re = x_ref[:, 0, :]
    im = x_ref[:, 1, :]
    local = jnp.sum(re * re + im * im, axis=1, keepdims=True)
    eye = lax.broadcasted_iota(jnp.int32, (span, 128), 0) == lax.broadcasted_iota(jnp.int32, (span, 128), 1)
    pbuf[0, pl.ds(me, 1), :] = jnp.sum(jnp.where(eye, local, 0.0), axis=0, keepdims=True)
    for p in range(pieces):
        for h in range(PIECE // 128):
            cols = slice(p * PIECE + h * 128, p * PIECE + (h + 1) * 128)
            buf[p, me, 0, h] = re[:, cols].astype(jnp.bfloat16)
            buf[p, me, 1, h] = im[:, cols].astype(jnp.bfloat16)
    pl.semaphore_wait(barrier, nf - 1 + n - 1)

    def share_copy(o, block):
        return pltpu.make_async_remote_copy(
            src_ref=pbuf.at[0, pl.ds(block, 1)], dst_ref=pbuf.at[0, pl.ds(block, 1)],
            send_sem=r_send.at[o], recv_sem=r_recv.at[o],
            device_id=(xor(me, o), mf), device_id_type=MESH)

    def power_copy(d):
        return pltpu.make_async_remote_copy(
            src_ref=pbuf.at[0], dst_ref=pbuf.at[d], send_sem=p_send.at[d], recv_sem=p_recv.at[d],
            device_id=(me, (mf + d) % nf), device_id_type=MESH)

    def own_copy(p, o):
        return pltpu.make_async_remote_copy(
            src_ref=buf.at[p, me], dst_ref=buf.at[p, me], send_sem=bulk_send.at[p, o], recv_sem=bulk_recv.at[p, o],
            device_id=(xor(me, o), mf), device_id_type=MESH)

    def pass_copy(p, o):
        block = xor(me, o)
        return pltpu.make_async_remote_copy(
            src_ref=buf.at[p, block], dst_ref=buf.at[p, block],
            send_sem=bulk_send.at[p, o + 1], recv_sem=bulk_recv.at[p, o + 1],
            device_id=(xor(me, 1), mf), device_id_type=MESH)

    def landed(p, o):
        block = xor(me, o)
        pltpu.make_async_remote_copy(
            src_ref=buf.at[p, block], dst_ref=buf.at[p, block],
            send_sem=bulk_send.at[p, o], recv_sem=bulk_recv.at[p, o],
            device_id=(xor(me, o), mf), device_id_type=MESH).wait_recv()

    for o in evens + [1] + list(range(3, n, 2)):
        share_copy(o, me).start()
    for p in range(pieces):
        for o in evens + [1]:
            own_copy(p, o).start()

    for load in loads[1:5]:
        load.wait()
    lag = [lag_ref[l] for l in range(nlag)]
    for turn in range(nlag):
        for l in range(turn % 2, nlag - 1, 2):
            lag[l], lag[l + 1] = jnp.minimum(lag[l], lag[l + 1]), jnp.maximum(lag[l], lag[l + 1])
    lag = [jnp.maximum(value, 1) for value in lag]

    def harmonics(count, lanes):
        r = lax.broadcasted_iota(jnp.int32, (count, lanes), 0)
        even_n = 2 * ((r + 1) // 2)
        even_s = jnp.where(r > 0, 1 - r % 2, 0)
        odd_n = 2 * (r // 2) + 1
        odd_s = r % 2
        return [(a.astype(jnp.float32), b.astype(jnp.float32)) for a, b in ((even_n, even_s), (odd_n, odd_s))]

    for c in range(rows // 128):
        index = (lax.broadcasted_iota(jnp.int32, (most, 128), 1) + c * 128).astype(jnp.float32)
        position = index - PERIOD * jnp.floor((index + 0.5) * (1.0 / PERIOD))
        for parity, (harmonic, quarter) in enumerate(harmonics(most, 128)):
            steps = harmonic * position
            steps = steps - PERIOD * jnp.floor((steps + 0.5) * (1.0 / PERIOD))
            base[parity, :, c * 128:(c + 1) * 128] = turn_cos(steps * (1.0 / PERIOD) - 0.25 * quarter)

    lane = lax.broadcasted_iota(jnp.int32, (1, 2 * NGRID), 1)
    level = (lane % NGRID).astype(jnp.float32)
    for k in range(nlag):
        for parity, (harmonic, quarter) in enumerate(harmonics(heads[k], 2 * NGRID)):
            turns = harmonic * (level * (1.0 / NGRID))
            turns = turns - jnp.round(turns)
            half = harmonic * lag[k].astype(jnp.float32) * (0.5 / PERIOD)
            half = half - jnp.round(half)
            value = turn_cos(turns + half + 0.25 * quarter)
            high = value.astype(jnp.bfloat16).astype(jnp.float32)
            start = starts[k] + parity * heads[k]
            wave[start:start + heads[k], :] = jnp.where(lane < NGRID, high, value - high).astype(jnp.bfloat16)

    rows_ref[0] = jnp.full((8, width), -1.0, jnp.float32)
    for c in range(rows // 128):
        ids = det_ref[c * 128:(c + 1) * 128].astype(jnp.float32)[None, :]
        rows_ref[0, :, c * 128:(c + 1) * 128] = jnp.broadcast_to(ids, (8, 128))
    det_row = rows_ref[0, 0:1, :]
    for v in range(1, LAGMAX + 1):
        shifted[v - 1:v, :] = pltpu.roll(det_row, width - v, 1)
    near = det_row[:, :rows]
    far = shifted[:, :rows]
    ndet = inter_ref.shape[0]
    gains = jnp.zeros((LAGMAX, rows), jnp.float32)
    for b in range(ndet):
        gain = jnp.zeros((1, rows), jnp.float32)
        for a in range(ndet):
            gain = jnp.where(near == a, inter_ref[a, b], gain)
        gains = jnp.where(far == b, gain, gains)
    weights[...] = gains

    for h in range(PIECE // 128):
        white[:, h, rows:rows + LAGMAX, :] = jnp.zeros((2, LAGMAX, 128), jnp.float32)

    def forward(p):
        for o in evens[::-1]:
            landed(p, o)
            pass_copy(p, o).start()

    for o in range(1, n):
        share_copy(o, xor(me, o)).wait_recv()
    for d in range(1, nf):
        power_copy(d).start()

    loads[5].wait()
    for k in range(nlag):
        for parity in range(2):
            start = starts[k] + parity * heads[k]
            picked[start:start + heads[k], :] = bess[lag[k] - 1, parity * most:parity * most + heads[k], :]
    grid_row = lax.broadcasted_iota(jnp.int32, (2 * NGRID, templ), 0) % NGRID
    pick_amplitude = (grid_row == tid_ref[0:1, :]).astype(jnp.float32).T.astype(jnp.bfloat16)
    pick_phase = (grid_row == tid_ref[1:2, :]).astype(jnp.float32).T.astype(jnp.bfloat16)
    contract = (((1,), (1,)), ((), ()))
    step = 256
    for c in range(total_rows // step):
        here = slice(c * step, (c + 1) * step)
        bessel_part = lax.dot_general(
            pick_amplitude, picked[here, :], contract, preferred_element_type=jnp.float32)
        wave_part = lax.dot_general(pick_phase, wave[here, :], contract, preferred_element_type=jnp.float32)
        product = bessel_part * wave_part
        for h in range(step // 128):
            factors[c * (step // 128) + h] = product[:, h * 128:(h + 1) * 128].astype(jnp.bfloat16)

    forward(0)

    total = pbuf[0]
    for d in range(1, nf):
        power_copy(d).wait_recv()
        total = total + pbuf[d]
    rates = lax.rsqrt(total * (1.0 / NBIN) + 1e-06)
    rates = jnp.where(lax.broadcasted_iota(jnp.int32, (n, 128), 1) < span, rates, 0.0)
    rates = jnp.concatenate([rates, jnp.zeros((n, width - 128), jnp.float32)], axis=1)
    rate_row = rates[0:1]
    for g in range(1, n):
        rate_row = rate_row + pltpu.roll(rates[g:g + 1], g * span, 1)
    for v in range(1, LAGMAX + 1):
        shifted[v - 1:v, :] = pltpu.roll(rate_row, width - v, 1)
    weights[...] = weights[...] * (rate_row[:, :rows] * shifted[:, :rows])
    for k in range(nlag):
        weight = weights[pl.ds(lag[k] - 1, 1), :]
        for parity in range(2):
            start = starts[k] + parity * heads[k]
            for c in range(rows // 128):
                cols = slice(c * 128, (c + 1) * 128)
                basis[c, start:start + heads[k], :] = (base[parity, :heads[k], cols] * weight[:, cols]).astype(jnp.bfloat16)

    def piece_step(p, carry):
        for o in range(1, n, 2):
            landed(p, o)

        for g in range(n):
            here = slice(g * span, (g + 1) * span)
            for c in range(2):
                for h in range(PIECE // 128):
                    white[c, h, here, :] = buf[p, g, c, h].astype(jnp.float32)
                    near_rows[c, h, here, :] = buf[p, g, c, h]

        for group in range(0, nlag, 1):
            if group == 2:
                @pl.when(p + 1 < pieces)
                def _():
                    forward(p + 1)

            slots = range(group, group + 1)
            sums = [[0.0, 0.0] for _ in slots]
            for first, last in [(lo, min(lo + 256, rows)) for lo in range(0, rows, 256)]:
                count = last - first
                a, b = [
                    jnp.concatenate([near_rows[part, h, first:last] for h in range(PIECE // 128)], axis=1)
                    for part in range(2)]
                for at, k in enumerate(slots):
                    there = pl.ds(lag[k] + first, count)
                    c, d = [
                        jnp.concatenate([white[part, h, there, :] for h in range(PIECE // 128)], axis=1).astype(jnp.bfloat16)
                        for part in range(2)]
                    for parity in range(2):
                        start = starts[k] + parity * heads[k]
                        both = a * d - b * c if parity else a * c + b * d
                        sums[at][parity] += jnp.dot(
                            jnp.concatenate(
                                [basis[t, start:start + heads[k], :] for t in range(first // 128, last // 128)], axis=1),
                            both, preferred_element_type=jnp.float32)
            for at, k in enumerate(slots):
                for parity in range(2):
                    start = starts[k] + parity * heads[k]
                    for h in range(PIECE // 128):
                        series[h, start:start + heads[k], :] = sums[at][parity][:, h * 128:(h + 1) * 128].astype(jnp.bfloat16)
        product = jnp.dot(
            jnp.concatenate([factors[c] for c in range(total_rows // 128)], axis=1),
            jnp.concatenate([series[h] for h in range(PIECE // 128)], axis=1), preferred_element_type=jnp.float32)
        out_ref[:, pl.ds(pl.multiple_of(p * PIECE, PIECE), PIECE)] = product.astype(out_ref.dtype)
        return carry

    lax.fori_loop(0, pieces, piece_step, 0)

    for d in range(1, nf):
        power_copy(d).wait_send()
    for o in range(1, n):
        share_copy(o, me).wait_send()

    def drain(p, carry):
        for o in evens + [1]:
            own_copy(p, o).wait_send()
        for o in evens:
            pass_copy(p, o).wait_send()
        return carry

    lax.fori_loop(0, pieces, drain, 0)


def shards(n, nf, sfts, detector_ids, intersection, lags, template_ids):
    span, _, width = sfts.shape
    rows = detector_ids.shape[0]
    nlag = lags.shape[0]
    templ = template_ids.shape[0]
    pieces = width // PIECE
    heads = harmonic_rows(nlag)
    most = max(heads)
    total_rows = 2 * sum(heads)
    table = jnp.asarray(bessel_table(most, 1.0 / math.sqrt(rows * nlag)))
    lanes = rows + 128
    vmem = pl.BlockSpec(memory_space=pltpu.VMEM)
    operands = [
        pltpu.with_memory_space_constraint(operand, pltpu.HBM)
        for operand in (sfts, detector_ids, intersection, lags, template_ids.T, table)
    ]
    return pl.pallas_call(
        functools.partial(kernel, n, nf, heads),
        out_shape=pltpu.VMEM((templ, width), jnp.float32),
        in_specs=[pl.BlockSpec(memory_space=pltpu.HBM)] * 6,
        out_specs=vmem,
        scratch_shapes=[
            pltpu.VMEM(sfts.shape, jnp.float32),
            pltpu.VMEM((rows,), jnp.int32),
            pltpu.SMEM(intersection.shape, jnp.float32),
            pltpu.SMEM((nlag,), jnp.int32),
            pltpu.VMEM((2, templ), jnp.int32),
            pltpu.VMEM((pieces, n, 2, PIECE // 128, span, 128), jnp.bfloat16),
            pltpu.VMEM((nf, n, 128), jnp.float32),
            pltpu.VMEM((1, 8, lanes), jnp.float32),
            pltpu.VMEM((LAGMAX, lanes), jnp.float32),
            pltpu.VMEM((LAGMAX, rows), jnp.float32),
            pltpu.VMEM((2, most, rows), jnp.float32),
            pltpu.VMEM((rows // 128, total_rows, 128), jnp.bfloat16),
            pltpu.VMEM(table.shape, jnp.bfloat16),
            pltpu.VMEM((total_rows, 2 * NGRID), jnp.bfloat16),
            pltpu.VMEM((total_rows, 2 * NGRID), jnp.bfloat16),
            pltpu.VMEM((total_rows // 128, templ, 128), jnp.bfloat16),
            pltpu.VMEM((2, PIECE // 128, rows + LAGMAX + 8, 128), jnp.float32),
            pltpu.VMEM((2, PIECE // 128, rows + 16, 128), jnp.bfloat16),
            pltpu.VMEM((PIECE // 128, total_rows, 128), jnp.bfloat16),
            pltpu.SemaphoreType.DMA((6,)),
            pltpu.SemaphoreType.DMA((pieces, n)),
            pltpu.SemaphoreType.DMA((pieces, n)),
            pltpu.SemaphoreType.DMA((nf,)),
            pltpu.SemaphoreType.DMA((nf,)),
            pltpu.SemaphoreType.DMA((n,)),
            pltpu.SemaphoreType.DMA((n,)),
        ],
        compiler_params=pltpu.CompilerParams(
            collective_id=0, has_side_effects=True, vmem_limit_bytes=48 * 1024 * 1024
        ),
    )(*operands)


def solution(mesh):
    n, nf = mesh.shape["tm"], mesh.shape["freq"]
    in_specs = (P("tm", None, "freq"), P(), P(), P(), P("tm", None))
    return jax.shard_map(
        functools.partial(shards, n, nf), mesh=mesh, in_specs=in_specs, out_specs=P("tm", "freq"), check_vma=False
    )
```

```python
import functools
import math

import jax
import jax.numpy as jnp
import numpy as np
from jax import lax
from jax.experimental import pallas as pl
from jax.experimental.pallas import tpu as pltpu
from jax.sharding import PartitionSpec as P

NBIN = 4096
LAGMAX = 16
NGRID = 64
PERIOD = 283
PIECE = 256
MESH = pl.DeviceIdType.MESH


def even_series(function, degree):
    nodes = np.cos(np.pi * (np.arange(64) + 0.5) / 64) * 0.125 + 0.125
    fit = np.polynomial.chebyshev.Chebyshev.fit(nodes, function(np.sqrt(nodes)), degree, domain=[0, 0.25])
    return [float(c) for c in fit.convert(kind=np.polynomial.Polynomial).coef]


COS_SERIES = even_series(lambda y: np.cos(2 * np.pi * y), 7)


def horner(series, z):
    value = jnp.full_like(z, series[-1])
    for coefficient in series[-2::-1]:
        value = value * z + coefficient
    return value


def turn_cos(turns):
    y = turns - jnp.round(turns)
    return horner(COS_SERIES, y * y)


def xor(index, bits):
    out = index
    bit = 1
    while bit <= bits:
        if bits & bit:
            out = out + bit - 2 * bit * ((index // bit) % 2)
        bit *= 2
    return out


def bessel(argument, count):
    turn = np.arange(1024) * (2 * np.pi / 1024)
    wave = np.exp(1j * argument[..., None] * np.sin(turn))
    return np.real(np.fft.fft(wave, axis=-1) / 1024)[..., :count]


def argument_of(lag):
    return (8.0 + 4.0 * np.arange(NGRID)) * 2.0 * np.sin(np.pi * lag / PERIOD)


def harmonic_rows(nlag):
    rows = []
    for k in range(nlag):
        values = np.abs(bessel(argument_of(LAGMAX - nlag + 1 + k), 256))
        last = int(np.nonzero(values.max(axis=0) > 1e-5)[0].max())
        rows.append(-(-(last + 1) // 16) * 16)
    return rows


def row_harmonics(count):
    r = np.arange(count)
    even_n, even_s = 2 * ((r + 1) // 2), ((r > 0) & (r % 2 == 0)).astype(int)
    odd_n, odd_s = 2 * (r // 2) + 1, r % 2
    return np.concatenate([even_n, odd_n]), np.concatenate([even_s, odd_s])


def bessel_table(count, scale):
    n, _ = row_harmonics(count)
    values = np.stack([bessel(argument_of(lag), 256) for lag in range(1, LAGMAX + 1)])
    sign = np.where(n == 0, 1.0, 2.0) * np.where((n // 2) % 2 == 0, 1.0, -1.0) * scale
    table = (values[:, :, n] * sign).transpose(0, 2, 1)
    high = table.astype(jnp.bfloat16)
    low = (table - high.astype(np.float64)).astype(jnp.bfloat16)
    return np.concatenate([high, low], axis=2)


def kernel(
    n, nf, heads,
    x_hbm, det_hbm, inter_hbm, lag_hbm, tid_hbm, bess_hbm, out_ref,
    x_ref, det_ref, inter_ref, lag_ref, tid_ref,
    buf, pbuf, rows_ref, shifted, weights, base, basis, bess, wave, picked, factors, white, near_rows, series, load_sem,
    bulk_send, bulk_recv, p_send, p_recv, r_send, r_recv,
):
    me = lax.axis_index("tm")
    mf = lax.axis_index("freq")
    span = x_ref.shape[0]
    rows = n * span
    nlag = lag_ref.shape[0]
    pieces = buf.shape[0]
    templ = tid_ref.shape[1]
    width = rows_ref.shape[2]
    most = base.shape[1]
    evens = sorted(range(2, n, 2), key=lambda o: -bin(o).count("1"))
    starts = [2 * sum(heads[:k]) for k in range(nlag + 1)]
    total_rows = starts[-1]

    loads = [
        pltpu.make_async_copy(source, target, load_sem.at[i])
        for i, (source, target) in enumerate([
            (x_hbm, x_ref), (lag_hbm, lag_ref), (det_hbm, det_ref), (tid_hbm, tid_ref), (inter_hbm, inter_ref),
            (bess_hbm, bess)])
    ]
    for load in loads:
        load.start()
    barrier = pltpu.get_barrier_semaphore()
    for d in range(1, nf):
        pl.semaphore_signal(barrier, inc=1, device_id=(me, (mf + d) % nf), device_id_type=MESH)
    for o in range(1, n):
        pl.semaphore_signal(barrier, inc=1, device_id=(xor(me, o), mf), device_id_type=MESH)

    loads[0].wait()
    re = x_ref[:, 0, :]
    im = x_ref[:, 1, :]
    local = jnp.sum(re * re + im * im, axis=1, keepdims=True)
    eye = lax.broadcasted_iota(jnp.int32, (span, 128), 0) == lax.broadcasted_iota(jnp.int32, (span, 128), 1)
    pbuf[0, pl.ds(me, 1), :] = jnp.sum(jnp.where(eye, local, 0.0), axis=0, keepdims=True)
    for p in range(pieces):
        for h in range(PIECE // 128):
            cols = slice(p * PIECE + h * 128, p * PIECE + (h + 1) * 128)
            buf[p, me, 0, h] = re[:, cols].astype(jnp.bfloat16)
            buf[p, me, 1, h] = im[:, cols].astype(jnp.bfloat16)
    pl.semaphore_wait(barrier, nf - 1 + n - 1)

    def share_copy(o, block):
        return pltpu.make_async_remote_copy(
            src_ref=pbuf.at[0, pl.ds(block, 1)], dst_ref=pbuf.at[0, pl.ds(block, 1)],
            send_sem=r_send.at[o], recv_sem=r_recv.at[o],
            device_id=(xor(me, o), mf), device_id_type=MESH)

    def power_copy(d):
        return pltpu.make_async_remote_copy(
            src_ref=pbuf.at[0], dst_ref=pbuf.at[d], send_sem=p_send.at[d], recv_sem=p_recv.at[d],
            device_id=(me, (mf + d) % nf), device_id_type=MESH)

    def own_copy(p, o):
        return pltpu.make_async_remote_copy(
            src_ref=buf.at[p, me], dst_ref=buf.at[p, me], send_sem=bulk_send.at[p, o], recv_sem=bulk_recv.at[p, o],
            device_id=(xor(me, o), mf), device_id_type=MESH)

    def pass_copy(p, o):
        block = xor(me, o)
        return pltpu.make_async_remote_copy(
            src_ref=buf.at[p, block], dst_ref=buf.at[p, block],
            send_sem=bulk_send.at[p, o + 1], recv_sem=bulk_recv.at[p, o + 1],
            device_id=(xor(me, 1), mf), device_id_type=MESH)

    def landed(p, o):
        block = xor(me, o)
        pltpu.make_async_remote_copy(
            src_ref=buf.at[p, block], dst_ref=buf.at[p, block],
            send_sem=bulk_send.at[p, o], recv_sem=bulk_recv.at[p, o],
            device_id=(xor(me, o), mf), device_id_type=MESH).wait_recv()

    for o in evens + [1] + list(range(3, n, 2)):
        share_copy(o, me).start()
    for p in range(pieces):
        for o in evens + [1]:
            own_copy(p, o).start()

    for load in loads[1:5]:
        load.wait()
    lag = [lag_ref[l] for l in range(nlag)]
    for turn in range(nlag):
        for l in range(turn % 2, nlag - 1, 2):
            lag[l], lag[l + 1] = jnp.minimum(lag[l], lag[l + 1]), jnp.maximum(lag[l], lag[l + 1])
    lag = [jnp.maximum(value, 1) for value in lag]

    def harmonics(count, lanes):
        r = lax.broadcasted_iota(jnp.int32, (count, lanes), 0)
        even_n = 2 * ((r + 1) // 2)
        even_s = jnp.where(r > 0, 1 - r % 2, 0)
        odd_n = 2 * (r // 2) + 1
        odd_s = r % 2
        return [(a.astype(jnp.float32), b.astype(jnp.float32)) for a, b in ((even_n, even_s), (odd_n, odd_s))]

    for c in range(rows // 128):
        index = (lax.broadcasted_iota(jnp.int32, (most, 128), 1) + c * 128).astype(jnp.float32)
        position = index - PERIOD * jnp.floor((index + 0.5) * (1.0 / PERIOD))
        for parity, (harmonic, quarter) in enumerate(harmonics(most, 128)):
            steps = harmonic * position
            steps = steps - PERIOD * jnp.floor((steps + 0.5) * (1.0 / PERIOD))
            base[parity, :, c * 128:(c + 1) * 128] = turn_cos(steps * (1.0 / PERIOD) - 0.25 * quarter)

    lane = lax.broadcasted_iota(jnp.int32, (1, 2 * NGRID), 1)
    level = (lane % NGRID).astype(jnp.float32)
    for k in range(nlag):
        for parity, (harmonic, quarter) in enumerate(harmonics(heads[k], 2 * NGRID)):
            turns = harmonic * (level * (1.0 / NGRID))
            turns = turns - jnp.round(turns)
            half = harmonic * lag[k].astype(jnp.float32) * (0.5 / PERIOD)
            half = half - jnp.round(half)
            value = turn_cos(turns + half + 0.25 * quarter)
            high = value.astype(jnp.bfloat16).astype(jnp.float32)
            start = starts[k] + parity * heads[k]
            wave[start:start + heads[k], :] = jnp.where(lane < NGRID, high, value - high).astype(jnp.bfloat16)

    rows_ref[0] = jnp.full((8, width), -1.0, jnp.float32)
    for c in range(rows // 128):
        ids = det_ref[c * 128:(c + 1) * 128].astype(jnp.float32)[None, :]
        rows_ref[0, :, c * 128:(c + 1) * 128] = jnp.broadcast_to(ids, (8, 128))
    det_row = rows_ref[0, 0:1, :]
    for v in range(1, LAGMAX + 1):
        shifted[v - 1:v, :] = pltpu.roll(det_row, width - v, 1)
    near = det_row[:, :rows]
    far = shifted[:, :rows]
    ndet = inter_ref.shape[0]
    gains = jnp.zeros((LAGMAX, rows), jnp.float32)
    for b in range(ndet):
        gain = jnp.zeros((1, rows), jnp.float32)
        for a in range(ndet):
            gain = jnp.where(near == a, inter_ref[a, b], gain)
        gains = jnp.where(far == b, gain, gains)
    weights[...] = gains

    for h in range(PIECE // 128):
        white[:, h, rows:rows + LAGMAX, :] = jnp.zeros((2, LAGMAX, 128), jnp.float32)

    def forward(p):
        for o in evens[::-1]:
            landed(p, o)
            pass_copy(p, o).start()

    for o in range(1, n):
        share_copy(o, xor(me, o)).wait_recv()
    for d in range(1, nf):
        power_copy(d).start()

    loads[5].wait()
    for k in range(nlag):
        for parity in range(2):
            start = starts[k] + parity * heads[k]
            picked[start:start + heads[k], :] = bess[lag[k] - 1, parity * most:parity * most + heads[k], :]
    grid_row = lax.broadcasted_iota(jnp.int32, (2 * NGRID, templ), 0) % NGRID
    pick_amplitude = (grid_row == tid_ref[0:1, :]).astype(jnp.float32).T.astype(jnp.bfloat16)
    pick_phase = (grid_row == tid_ref[1:2, :]).astype(jnp.float32).T.astype(jnp.bfloat16)
    contract = (((1,), (1,)), ((), ()))
    step = 256
    for c in range(total_rows // step):
        here = slice(c * step, (c + 1) * step)
        bessel_part = lax.dot_general(
            pick_amplitude, picked[here, :], contract, preferred_element_type=jnp.float32)
        wave_part = lax.dot_general(pick_phase, wave[here, :], contract, preferred_element_type=jnp.float32)
        product = bessel_part * wave_part
        for h in range(step // 128):
            factors[c * (step // 128) + h] = product[:, h * 128:(h + 1) * 128].astype(jnp.bfloat16)

    forward(0)

    total = pbuf[0]
    for d in range(1, nf):
        power_copy(d).wait_recv()
        total = total + pbuf[d]
    rates = lax.rsqrt(total * (1.0 / NBIN) + 1e-06)
    rates = jnp.where(lax.broadcasted_iota(jnp.int32, (n, 128), 1) < span, rates, 0.0)
    rates = jnp.concatenate([rates, jnp.zeros((n, width - 128), jnp.float32)], axis=1)
    rate_row = rates[0:1]
    for g in range(1, n):
        rate_row = rate_row + pltpu.roll(rates[g:g + 1], g * span, 1)
    for v in range(1, LAGMAX + 1):
        shifted[v - 1:v, :] = pltpu.roll(rate_row, width - v, 1)
    weights[...] = weights[...] * (rate_row[:, :rows] * shifted[:, :rows])
    for k in range(nlag):
        weight = weights[pl.ds(lag[k] - 1, 1), :]
        for parity in range(2):
            start = starts[k] + parity * heads[k]
            for c in range(rows // 128):
                cols = slice(c * 128, (c + 1) * 128)
                basis[c, start:start + heads[k], :] = (base[parity, :heads[k], cols] * weight[:, cols]).astype(jnp.bfloat16)

    def piece_step(p, carry):
        for o in range(1, n, 2):
            landed(p, o)

        for g in range(n):
            here = slice(g * span, (g + 1) * span)
            for c in range(2):
                for h in range(PIECE // 128):
                    white[c, h, here, :] = buf[p, g, c, h].astype(jnp.float32)
                    near_rows[c, h, here, :] = buf[p, g, c, h]

        for group in range(0, nlag, 2):
            if group == 2:
                @pl.when(p + 1 < pieces)
                def _():
                    forward(p + 1)

            slots = range(group, group + 2)
            sums = [[0.0, 0.0] for _ in slots]
            for first, last in [(lo, min(lo + 256, rows)) for lo in range(0, rows, 256)]:
                count = last - first
                a, b = [
                    jnp.concatenate([near_rows[part, h, first:last] for h in range(PIECE // 128)], axis=1)
                    for part in range(2)]
                for at, k in enumerate(slots):
                    there = pl.ds(lag[k] + first, count)
                    c, d = [
                        jnp.concatenate([white[part, h, there, :] for h in range(PIECE // 128)], axis=1).astype(jnp.bfloat16)
                        for part in range(2)]
                    for parity in range(2):
                        start = starts[k] + parity * heads[k]
                        both = a * d - b * c if parity else a * c + b * d
                        sums[at][parity] += jnp.dot(
                            jnp.concatenate(
                                [basis[t, start:start + heads[k], :] for t in range(first // 128, last // 128)], axis=1),
                            both, preferred_element_type=jnp.float32)
            for at, k in enumerate(slots):
                for parity in range(2):
                    start = starts[k] + parity * heads[k]
                    for h in range(PIECE // 128):
                        series[h, start:start + heads[k], :] = sums[at][parity][:, h * 128:(h + 1) * 128].astype(jnp.bfloat16)
        product = jnp.dot(
            jnp.concatenate([factors[c] for c in range(total_rows // 128)], axis=1),
            jnp.concatenate([series[h] for h in range(PIECE // 128)], axis=1), preferred_element_type=jnp.float32)
        out_ref[:, pl.ds(pl.multiple_of(p * PIECE, PIECE), PIECE)] = product.astype(out_ref.dtype)
        return carry

    lax.fori_loop(0, pieces, piece_step, 0)

    for d in range(1, nf):
        power_copy(d).wait_send()
    for o in range(1, n):
        share_copy(o, me).wait_send()

    def drain(p, carry):
        for o in evens + [1]:
            own_copy(p, o).wait_send()
        for o in evens:
            pass_copy(p, o).wait_send()
        return carry

    lax.fori_loop(0, pieces, drain, 0)


def shards(n, nf, sfts, detector_ids, intersection, lags, template_ids):
    span, _, width = sfts.shape
    rows = detector_ids.shape[0]
    nlag = lags.shape[0]
    templ = template_ids.shape[0]
    pieces = width // PIECE
    heads = harmonic_rows(nlag)
    most = max(heads)
    total_rows = 2 * sum(heads)
    table = jnp.asarray(bessel_table(most, 1.0 / math.sqrt(rows * nlag)))
    lanes = rows + 128
    vmem = pl.BlockSpec(memory_space=pltpu.VMEM)
    operands = [
        pltpu.with_memory_space_constraint(operand, pltpu.HBM)
        for operand in (sfts, detector_ids, intersection, lags, template_ids.T, table)
    ]
    return pl.pallas_call(
        functools.partial(kernel, n, nf, heads),
        out_shape=pltpu.VMEM((templ, width), jnp.float32),
        in_specs=[pl.BlockSpec(memory_space=pltpu.HBM)] * 6,
        out_specs=vmem,
        scratch_shapes=[
            pltpu.VMEM(sfts.shape, jnp.float32),
            pltpu.VMEM((rows,), jnp.int32),
            pltpu.SMEM(intersection.shape, jnp.float32),
            pltpu.SMEM((nlag,), jnp.int32),
            pltpu.VMEM((2, templ), jnp.int32),
            pltpu.VMEM((pieces, n, 2, PIECE // 128, span, 128), jnp.bfloat16),
            pltpu.VMEM((nf, n, 128), jnp.float32),
            pltpu.VMEM((1, 8, lanes), jnp.float32),
            pltpu.VMEM((LAGMAX, lanes), jnp.float32),
            pltpu.VMEM((LAGMAX, rows), jnp.float32),
            pltpu.VMEM((2, most, rows), jnp.float32),
            pltpu.VMEM((rows // 128, total_rows, 128), jnp.bfloat16),
            pltpu.VMEM(table.shape, jnp.bfloat16),
            pltpu.VMEM((total_rows, 2 * NGRID), jnp.bfloat16),
            pltpu.VMEM((total_rows, 2 * NGRID), jnp.bfloat16),
            pltpu.VMEM((total_rows // 128, templ, 128), jnp.bfloat16),
            pltpu.VMEM((2, PIECE // 128, rows + LAGMAX + 8, 128), jnp.float32),
            pltpu.VMEM((2, PIECE // 128, rows + 16, 128), jnp.bfloat16),
            pltpu.VMEM((PIECE // 128, total_rows, 128), jnp.bfloat16),
            pltpu.SemaphoreType.DMA((6,)),
            pltpu.SemaphoreType.DMA((pieces, n)),
            pltpu.SemaphoreType.DMA((pieces, n)),
            pltpu.SemaphoreType.DMA((nf,)),
            pltpu.SemaphoreType.DMA((nf,)),
            pltpu.SemaphoreType.DMA((n,)),
            pltpu.SemaphoreType.DMA((n,)),
        ],
        compiler_params=pltpu.CompilerParams(
            collective_id=0, has_side_effects=True, vmem_limit_bytes=48 * 1024 * 1024
        ),
    )(*operands)


def solution(mesh):
    n, nf = mesh.shape["tm"], mesh.shape["freq"]
    in_specs = (P("tm", None, "freq"), P(), P(), P(), P("tm", None))
    return jax.shard_map(
        functools.partial(shards, n, nf), mesh=mesh, in_specs=in_specs, out_specs=P("tm", "freq"), check_vma=False
    )
```
